8 devices in a mesh: dp: 1 (over z), tp: 8 (over x, y, core).
Axes of the slice: x: 2, y: 2, z: 1, core: 2. Of those that a mesh axis runs over, the one named last changes fastest.
Arguments:
- x: bfloat16 [1, 2048, 7168], P('dp', 'tp')
- dy: bfloat16 [1, 2048, 7168], P('dp', 'tp')
- wq: bfloat16 [7168, 7168], P(None, 'tp')
- wk: bfloat16 [7168, 1024], P(None, 'tp')
- wv: bfloat16 [7168, 1024], P(None, 'tp')
- wo: bfloat16 [7168, 7168], P('tp')
- w_gate: bfloat16 [7168, 20480], P(None, 'tp')
- w_up: bfloat16 [7168, 20480], P(None, 'tp')
- w_down: bfloat16 [20480, 7168], P('tp')
Outputs:
- output 1: bfloat16 [1, 2048, 7168], P('dp', 'tp')
- output 2: bfloat16 [7168, 7168], P('dp', 'tp')
- output 3: bfloat16 [7168, 1024], P('dp', 'tp')
- output 4: bfloat16 [7168, 1024], P('dp', 'tp')
- output 5: bfloat16 [7168, 7168], P(('dp', 'tp'))
- output 6: bfloat16 [7168, 20480], P('dp', 'tp')
- output 7: bfloat16 [7168, 20480], P('dp', 'tp')
- output 8: bfloat16 [20480, 7168], P(('dp', 'tp'))
All inputs are finite; a program needn't handle non-finite values.
Results may differ from the reference program's by a relative error of at most 0.024.
Values are sent between devices in bfloat16 or wider.
A program may use at most 2 GiB of HBM per device.

```python
import jax
import jax.numpy as jnp
from jax import lax

SEQUENCES = 1
TOKENS = 2048
D = 7168
HEADS = 56
KV_HEADS = 8
HEAD = 128
FF = 20480
THETA = 10000
NAMES = ("wq", "wk", "wv", "wo", "w_gate", "w_up", "w_down")
SHAPES = {
    "wq": (D, HEADS * HEAD),
    "wk": (D, KV_HEADS * HEAD),
    "wv": (D, KV_HEADS * HEAD),
    "wo": (HEADS * HEAD, D),
    "w_gate": (D, FF),
    "w_up": (D, FF),
    "w_down": (FF, D),
}


def bump(key, n, height):
    away = (jnp.arange(n, dtype=jnp.int32) - jax.random.randint(key, (), 0, n, jnp.int32)) % n
    return jnp.where(away < n // 8, height, 1.0)


def together(key, own, strength):
    shared = jax.random.normal(key, own.shape[1:], jnp.float32)
    return (own + strength * shared) * lax.rsqrt(1 + strength * strength)


def setup_inputs(seed: int = 0, part: int = 0) -> dict:
    kx, kdy, ka, kb, kz, kf, kh, kl, *kw = jax.random.split(jax.random.key(seed), 8 + len(NAMES))
    kx, kdy, ka, kb = (jax.random.fold_in(k, part) for k in (kx, kdy, ka, kb))
    shape = (SEQUENCES, TOKENS, D)
    much_x, much_dy = jax.random.uniform(kz, (2,), jnp.float32, 0.0, 1.0)
    loud = 2.0 ** jax.random.uniform(jax.random.fold_in(kz, 1), (), jnp.float32, -1.0, 2.0)
    halves = 2.0 ** jax.random.uniform(kl, (2,), jnp.float32, -1.0, 1.0)
    times = {"wq": 1.0, "wk": 1.0, "wv": 2.0, "wo": halves[0], "w_gate": 1.0, "w_up": bump(kh, FF, 4.0), "w_down": halves[1]}
    x = together(ka, jax.random.normal(kx, shape, jnp.float32), much_x) * bump(kf, D, 4.0)
    dy = together(kb, jax.random.normal(kdy, shape, jnp.float32), much_dy)
    drawn = {"x": x.astype(jnp.bfloat16), "dy": (loud * dy * (SEQUENCES * TOKENS) ** -0.5).astype(jnp.bfloat16)}
    for key, name in zip(kw, NAMES, strict=True):
        drawn[name] = (jax.random.normal(key, SHAPES[name], jnp.float32) * SHAPES[name][0] ** -0.5 * times[name]).astype(jnp.bfloat16)
    return drawn


def matmul(a, w):
    return jnp.dot(a, w, preferred_element_type=jnp.float32).astype(jnp.bfloat16)


def normed(h):
    wide = h.astype(jnp.float32)
    scale = lax.rsqrt(jnp.mean(wide**2, -1, keepdims=True) + 1e-6)
    return (wide * scale).astype(jnp.bfloat16)


def turned(t, theta):
    half = t.shape[-1] // 2
    angle = jnp.arange(t.shape[0], dtype=jnp.float32)[:, None] * theta ** (-jnp.arange(half, dtype=jnp.float32) / half)
    cos, sin = jnp.cos(angle)[:, None], jnp.sin(angle)[:, None]
    a, b = t[..., :half].astype(jnp.float32), t[..., half:].astype(jnp.float32)
    return jnp.concatenate([a * cos - b * sin, b * cos + a * sin], -1).astype(jnp.bfloat16)


def seen_by(q, k, v):
    tokens, kv = q.shape[0], k.shape[1]
    q = q.reshape(tokens, kv, -1, q.shape[-1])
    scores = jnp.einsum("tgsd,ugd->gstu", q.astype(jnp.float32), k.astype(jnp.float32)) * q.shape[-1] ** -0.5
    place = jnp.arange(tokens)
    weights = jax.nn.softmax(jnp.where(place[:, None] >= place, scores, -jnp.inf), -1).astype(jnp.bfloat16)
    return jnp.einsum("gstu,ugd->tgsd", weights.astype(jnp.float32), v.astype(jnp.float32)).astype(jnp.bfloat16).reshape(tokens, -1)


def layer(h, w):
    a = normed(h)
    q, k = (turned(matmul(a, w[name]).reshape(h.shape[0], -1, HEAD), THETA) for name in ("wq", "wk"))
    h = h + matmul(seen_by(q, k, matmul(a, w["wv"]).reshape(h.shape[0], -1, HEAD)), w["wo"])
    b = normed(h)
    gate = jnp.dot(b, w["w_gate"], preferred_element_type=jnp.float32)
    up = jnp.dot(b, w["w_up"], preferred_element_type=jnp.float32)
    return h + matmul((jax.nn.silu(gate) * up).astype(jnp.bfloat16), w["w_down"])


def reference(x, dy, wq, wk, wv, wo, w_gate, w_up, w_down):
    weights = dict(zip(NAMES, (wq, wk, wv, wo, w_gate, w_up, w_down), strict=True))

    def take(so_far, sequence):
        h, by_y = sequence
        _, back = jax.vjp(lambda w, h: layer(h, w), weights, h)
        by_weights, by_h = back(by_y)
        return jax.tree.map(lambda total, term: total + term.astype(jnp.float32), so_far, by_weights), by_h

    none_yet = {name: jnp.zeros(w.shape, jnp.float32) for name, w in weights.items()}
    by_weights, by_x = lax.scan(take, none_yet, (x, dy))
    return (by_x, *(by_weights[name].astype(jnp.bfloat16) for name in NAMES))
```

```python
import functools

import jax
import jax.numpy as jnp
from jax import lax
from jax.experimental import pallas as pl
from jax.experimental.pallas import tpu as pltpu

NEG = -1e30
HIDDEN = 2 * NEG
LOG2E = 1.4426950408889634
VMEM = 56 * 2**20
STRIP = 512
HEAD = 128
BF = jnp.bfloat16
F32 = jnp.float32


def _fit(size, want, unit=128):
    return max(n for n in range(unit, max(min(want, size), unit) + 1, unit) if size % n == 0)


def _dot(a, b, ca, cb):
    return lax.dot_general(a, b, (((ca,), (cb,)), ((), ())), preferred_element_type=F32)


def _gap(bk, cols, bq):
    return lax.rem(lax.broadcasted_iota(jnp.int32, (bk, cols), 1), bq) - lax.broadcasted_iota(jnp.int32, (bk, cols), 0)


def _turn(t, cos, sin):
    wide = t.astype(F32)
    return (wide * cos + pltpu.roll(wide, HEAD // 2, 1) * sin).astype(BF)


def _runs(size, own, rows):
    return [(n * own + p * rows, p, n * rows) for n in range(size // own) for p in range(own // rows)]


def _load_keys(kv, cos_ref, sin_ref, k_s, v_s, own, rows):
    for at, p, there in _runs(k_s.shape[0], own, rows):
        here = slice(at, at + rows)
        k_s[here, :] = _turn(kv[2 * p][there : there + rows, :], cos_ref[here, :], sin_ref[here, :])
        v_s[here, :] = kv[2 * p + 1][there : there + rows, :]


def _load_queries(qs, cos_ref, sin_ref, q_s, bq, own, rows):
    first = pl.program_id(0) * bq
    for at, p, there in _runs(bq, own, rows):
        here = pl.ds(first + at, rows)
        cos, sin = cos_ref[here, :], sin_ref[here, :]
        for n in range(q_s.shape[0] // bq):
            q_s[n * bq + at : n * bq + at + rows, :] = _turn(qs[p][there : there + rows, n * HEAD : (n + 1) * HEAD], cos, sin)


def _row(ref):
    return jnp.concatenate([ref[n : n + 1, :] for n in range(ref.shape[0])], axis=1)


def _blocks(bq, bk, block):
    first = pl.program_id(0) * bq
    whole, last = lax.div(first + 1, bk), lax.div(first + bq - 1 + bk, bk)
    lax.fori_loop(0, whole, lambda j, _: block(j, False), None)
    lax.fori_loop(whole, last, lambda j, _: block(j, True), None)


def _forward(*refs, pieces, own, scale, bq, bk):
    qs, kv = refs[:pieces], refs[pieces : 3 * pieces]
    cos_ref, sin_ref = refs[3 * pieces : 3 * pieces + 2]
    outs, (lse_ref, q_s, k_s, v_s, top_s, mix_s, gap_s) = refs[3 * pieces + 2 : 4 * pieces + 2], refs[4 * pieces + 2 :]
    rows, g, cols = own // pieces, q_s.shape[0] // bq, q_s.shape[0]
    e = scale * LOG2E
    wide = _fit(cols, STRIP)
    strips = range(0, cols, wide)
    first_query = pl.program_id(0) * bq

    @pl.when(pl.program_id(0) == 0)
    def _():
        gap_s[...] = _gap(bk, cols, bq)
        _load_keys(kv, cos_ref, sin_ref, k_s, v_s, own, rows)

    _load_queries(qs, cos_ref, sin_ref, q_s, bq, own, rows)
    top_s[...] = jnp.full_like(top_s, NEG)
    mix_s[...] = jnp.zeros_like(mix_s)
    ones = jnp.ones((8, bk), BF)

    def block(j, masked):
        here = pl.ds(j * bk, bk)
        scores = [_dot(k_s[here, :], q_s[at : at + wide, :], 1, 1) for at in strips]
        ok = gap_s[...] >= j * bk - first_query if masked else None
        weights, keeps = [], []
        for at, s in zip(strips, scores):
            if masked:
                s = jnp.where(ok[:, at : at + wide], s, HIDDEN)
            old = top_s[:, at : at + wide]
            top = jnp.maximum(old, s.max(axis=0, keepdims=True))
            top_s[:, at : at + wide] = top
            weights.append(jnp.exp2((s - top) * e).astype(BF))
            keeps.append(jnp.exp2((old - top) * e))
        for at, p, keep in zip(strips, weights, keeps):
            values = jnp.concatenate([v_s[here, :].T, ones], axis=0)
            mix_s[:, at : at + wide] = mix_s[:, at : at + wide] * keep + _dot(values, p, 1, 0)

    _blocks(bq, bk, block)
    total = mix_s[HEAD : HEAD + 1, :]
    out = (mix_s[:HEAD, :] * (1 / total)).T.astype(BF)
    for at, p, there in _runs(bq, own, rows):
        for n in range(g):
            outs[p][there : there + rows, n * HEAD : (n + 1) * HEAD] = out[n * bq + at : n * bq + at + rows, :]
    lse = top_s[...] * scale + jnp.log(total)
    for n in range(g):
        lse_ref[n : n + 1, :] = lse[:, n * bq : (n + 1) * bq]


def _cost(g, tokens, dots):
    return pl.CostEstimate(flops=g * tokens * tokens * HEAD * dots, transcendentals=g * tokens * tokens // 2, bytes_accessed=8 * g * tokens * HEAD)


def _given(qkv, g, bq, tokens):
    share, size = bq // len(qkv), qkv[0].shape[0]
    specs = [pl.BlockSpec((share, g * HEAD), lambda i: (i, 0))] * len(qkv)
    specs += [pl.BlockSpec((size, HEAD), lambda i: (0, g)), pl.BlockSpec((size, HEAD), lambda i: (0, g + 1))] * len(qkv)
    return specs + [pl.BlockSpec((tokens, HEAD), lambda i: (0, 0))] * 2


def attend(qkv, cos, sin, own, bq=512, bk=512):
    pieces, tokens = len(qkv), cos.shape[0]
    g = qkv[0].shape[1] // HEAD - 2
    cols, share = g * bq, bq // pieces
    *heads, lse = pl.pallas_call(
        functools.partial(_forward, pieces=pieces, own=own, scale=HEAD**-0.5, bq=bq, bk=bk),
        grid=(tokens // bq,), in_specs=_given(qkv, g, bq, tokens),
        out_specs=[pl.BlockSpec((share, g * HEAD), lambda i: (i, 0))] * pieces + [pl.BlockSpec((g, bq), lambda i: (0, i))],
        out_shape=[jax.ShapeDtypeStruct((t.shape[0], g * HEAD), BF) for t in qkv] + [jax.ShapeDtypeStruct((g, tokens), F32)],
        scratch_shapes=[pltpu.VMEM((cols, HEAD), BF), pltpu.VMEM((tokens, HEAD), BF), pltpu.VMEM((tokens, HEAD), BF), pltpu.VMEM((1, cols), F32),
                        pltpu.VMEM((HEAD + 8, cols), F32), pltpu.VMEM((bk, cols), jnp.int32)],
        compiler_params=pltpu.CompilerParams(dimension_semantics=("arbitrary",), vmem_limit_bytes=VMEM),
        cost_estimate=_cost(g, tokens, 2), name="attend")(*qkv, *(t for t in qkv for _ in (0, 1)), cos, sin)
    return heads, lse


def _backward(*refs, pieces, own, scale, bq, bk):
    qs, kv = refs[:pieces], refs[pieces : 3 * pieces]
    cos_ref, sin_ref = refs[3 * pieces : 3 * pieces + 2]
    d_heads, heads = refs[3 * pieces + 2 : 4 * pieces + 2], refs[4 * pieces + 2 : 5 * pieces + 2]
    lse_ref, outs = refs[5 * pieces + 2], refs[5 * pieces + 3 : 6 * pieces + 3]
    q_s, k_s, v_s, do_s, delta_s, dq_s, dk_s, dv_s, gap_s = refs[6 * pieces + 3 :]
    rows, g, cols = own // pieces, q_s.shape[0] // bq, q_s.shape[0]
    e = scale * LOG2E
    wide = _fit(cols, STRIP)
    strips = range(0, cols, wide)
    step = pl.program_id(0)
    first_query = step * bq

    @pl.when(step == 0)
    def _():
        gap_s[...] = _gap(bk, cols, bq)
        _load_keys(kv, cos_ref, sin_ref, k_s, v_s, own, rows)
        dk_s[...] = jnp.zeros_like(dk_s)
        dv_s[...] = jnp.zeros_like(dv_s)

    _load_queries(qs, cos_ref, sin_ref, q_s, bq, own, rows)
    for n in range(g):
        for at, p, there in _runs(bq, own, rows):
            out, d_out = (t[p][there : there + rows, n * HEAD : (n + 1) * HEAD] for t in (heads, d_heads))
            here = slice(n * bq + at, n * bq + at + rows)
            do_s[here, :] = d_out
            delta_s[:, here] = (d_out.astype(F32) * out.astype(F32)).T.sum(axis=0, keepdims=True)
    dq_s[...] = jnp.zeros_like(dq_s)
    lses = _row(lse_ref) * LOG2E

    def block(j, masked):
        here = pl.ds(j * bk, bk)
        part_q = [q_s[at : at + wide, :] for at in strips]
        part_do = [do_s[at : at + wide, :] for at in strips]
        scores = [_dot(k_s[here, :], x, 1, 1) for x in part_q]
        dps = [_dot(v_s[here, :], x, 1, 1) for x in part_do]
        ok = gap_s[...] >= j * bk - first_query if masked else None
        for n, at in enumerate(strips):
            p = jnp.exp2(scores[n] * e - lses[:, at : at + wide])
            if masked:
                p = jnp.where(ok[:, at : at + wide], p, 0.0)
            ds = (p * (dps[n] - delta_s[:, at : at + wide])).astype(BF)
            dv_s[here, :] += _dot(p.astype(BF), part_do[n], 1, 0)
            dk_s[here, :] += _dot(ds, part_q[n], 1, 0)
            dq_s[:, at : at + wide] += _dot(k_s[here, :].T, ds, 1, 0)

    _blocks(bq, bk, block)
    dq = (dq_s[...] * scale).T.astype(BF)
    share = bq // pieces
    for at, p, there in _runs(bq, own, rows):
        here = pl.ds(first_query + at, rows)
        cos, sin = cos_ref[here, :], sin_ref[here, :]
        for n in range(g):
            outs[p][pl.ds(step * share + there, rows), n * HEAD : (n + 1) * HEAD] = _turn(dq[n * bq + at : n * bq + at + rows, :], cos, -sin)

    @pl.when(step == pl.num_programs(0) - 1)
    def _():
        for at, p, there in _runs(dk_s.shape[0], own, rows):
            here = slice(at, at + rows)
            dk = (dk_s[here, :] * scale).astype(BF)
            outs[p][there : there + rows, g * HEAD : (g + 1) * HEAD] = _turn(dk, cos_ref[here, :], -sin_ref[here, :])
            outs[p][there : there + rows, (g + 1) * HEAD :] = dv_s[here, :].astype(BF)


def attend_bwd(qkv, cos, sin, d_heads, heads, lse, own, bq=256, bk=512):
    pieces, tokens = len(qkv), cos.shape[0]
    g = qkv[0].shape[1] // HEAD - 2
    cols, share = g * bq, bq // pieces
    whole = pl.BlockSpec(qkv[0].shape, lambda i: (0, 0))
    return pl.pallas_call(
        functools.partial(_backward, pieces=pieces, own=own, scale=HEAD**-0.5, bq=bq, bk=bk),
        grid=(tokens // bq,),
        in_specs=_given(qkv, g, bq, tokens) + [pl.BlockSpec((share, g * HEAD), lambda i: (i, 0))] * (2 * pieces) + [pl.BlockSpec((g, bq), lambda i: (0, i))],
        out_specs=[whole] * pieces, out_shape=[jax.ShapeDtypeStruct(t.shape, BF) for t in qkv],
        scratch_shapes=[pltpu.VMEM((cols, HEAD), BF), pltpu.VMEM((tokens, HEAD), BF), pltpu.VMEM((tokens, HEAD), BF), pltpu.VMEM((cols, HEAD), BF),
                        pltpu.VMEM((1, cols), F32), pltpu.VMEM((HEAD, cols), F32), pltpu.VMEM((tokens, HEAD), F32), pltpu.VMEM((tokens, HEAD), F32),
                        pltpu.VMEM((bk, cols), jnp.int32)],
        compiler_params=pltpu.CompilerParams(dimension_semantics=("arbitrary",), vmem_limit_bytes=VMEM),
        cost_estimate=_cost(g, tokens, 5), name="attend_bwd")(*qkv, *(t for t in qkv for _ in (0, 1)), cos, sin, *d_heads, *heads, lse)


from jax.sharding import PartitionSpec as P

THETA = 10000
GRANT = 62 * 2**20


def normed(h):
    wide = h.astype(F32)
    scale = lax.rsqrt(jnp.mean(wide**2, -1, keepdims=True) + 1e-6)
    return (wide * scale).astype(BF)


def turn_by(tokens):
    half = HEAD // 2
    angle = jnp.arange(tokens, dtype=F32)[:, None] * THETA ** (-jnp.arange(half, dtype=F32) / half)
    cos, sin = jnp.cos(angle), jnp.sin(angle)
    return jnp.concatenate([cos, cos], 1), jnp.concatenate([-sin, sin], 1)


def mm(a, b, ca=1, cb=0):
    return _dot(a, b, ca, cb).astype(BF)


def _matmul_cost(m, n, k, times=1):
    return pl.CostEstimate(flops=2 * m * n * k * times, transcendentals=0, bytes_accessed=2 * times * (m * k + k * n + m * n))


def gated(b, w_gate, w_up, d_hidden, name, tm=512, tn=512):
    t, d = b.shape
    f = w_gate.shape[1]
    tm, tn = _fit(t, tm), _fit(f, tn)

    def kernel(b_ref, wg_ref, wu_ref, dh_ref, h_ref, dg_ref, du_ref):
        gate = jnp.dot(b_ref[...], wg_ref[...], preferred_element_type=F32)
        up = jnp.dot(b_ref[...], wu_ref[...], preferred_element_type=F32)
        dh = dh_ref[...].astype(F32)
        s = jax.nn.sigmoid(gate)
        act = gate * s
        h_ref[...] = (act * up).astype(BF)
        du_ref[...] = (dh * act).astype(BF)
        dg_ref[...] = (dh * up * (s + act * (1 - s))).astype(BF)

    out = pl.BlockSpec((tm, tn), lambda i, j: (i, j))
    w = pl.BlockSpec((d, tn), lambda i, j: (0, j))
    return pl.pallas_call(
        kernel, grid=(t // tm, f // tn), in_specs=[pl.BlockSpec((tm, d), lambda i, j: (i, 0)), w, w, out], out_specs=[out] * 3,
        out_shape=[jax.ShapeDtypeStruct((t, f), BF)] * 3, cost_estimate=_matmul_cost(t, f, d, 2), name=name,
        compiler_params=pltpu.CompilerParams(vmem_limit_bytes=GRANT, dimension_semantics=("parallel", "arbitrary")))(b, w_gate, w_up, d_hidden)


def back_through(pairs, name, tm=1024, tn=512):
    t, f = pairs[0][0].shape
    d = pairs[0][1].shape[0]
    n = len(pairs)
    tm, tn = _fit(t, tm), _fit(d, tn)

    def kernel(*refs):
        total = None
        for g, w in zip(refs[:n], refs[n : 2 * n]):
            term = _dot(g[...], w[...], 1, 1)
            total = term if total is None else total + term
        refs[2 * n][...] = total.astype(BF)

    return pl.pallas_call(
        kernel, grid=(t // tm, d // tn),
        in_specs=[pl.BlockSpec((tm, f), lambda i, j: (i, 0))] * n + [pl.BlockSpec((tn, f), lambda i, j: (j, 0))] * n,
        out_specs=pl.BlockSpec((tm, tn), lambda i, j: (i, j)), out_shape=jax.ShapeDtypeStruct((t, d), BF),
        cost_estimate=_matmul_cost(t, d, f, n), name=name,
        compiler_params=pltpu.CompilerParams(vmem_limit_bytes=GRANT, dimension_semantics=("parallel", "arbitrary")))(
            *(g for g, _ in pairs), *(w for _, w in pairs))


def weight_grads(pieces, lists, name, tm, tn=None):
    c, (t, m) = len(pieces), pieces[0].shape
    k = len(lists)
    widths = [bs[0][2] if isinstance(bs[0], tuple) else bs[0].shape[1] for bs in lists]
    tm = _fit(m, tm)
    tns = widths if tn is None else [_fit(n, tn) for n in widths]

    def kernel(*refs):
        ours, theirs, outs = refs[:c], refs[c : c + c * k], refs[c + c * k :]
        for l, out in enumerate(outs):
            total = None
            for i in range(c):
                term = _dot(ours[i][...], theirs[l * c + i][...], 0, 0)
                total = term if total is None else total + term
            out[...] = total.astype(BF)

    specs, given = [pl.BlockSpec((t, tm), lambda j, i: (0, i))] * c, list(pieces)
    for b, tn in ((b, tn) for bs, tn in zip(lists, tns) for b in bs):
        if not isinstance(b, tuple):
            specs.append(pl.BlockSpec((t, tn), lambda j, i: (0, j)))
            given.append(b)
        else:
            specs.append(pl.BlockSpec((t, tn), lambda j, i, at=b[1] // tn: (0, at)))
            given.append(b[0])
    return pl.pallas_call(
        kernel, grid=(widths[0] // tns[0], m // tm), in_specs=specs, out_specs=[pl.BlockSpec((tm, tn), lambda j, i: (i, j)) for tn in tns],
        out_shape=[jax.ShapeDtypeStruct((m, n), BF) for n in widths], cost_estimate=_matmul_cost(m, sum(widths), c * t), name=name,
        compiler_params=pltpu.CompilerParams(vmem_limit_bytes=GRANT, dimension_semantics=("parallel", "arbitrary")))(*given)


def after(value, *others):
    return lax.optimization_barrier((value, *others))[0]


def gather(rows):
    return lax.all_gather(rows, "tp", axis=0, tiled=True)


def scatter(terms):
    return lax.psum_scatter(terms, "tp", scatter_dimension=0, tiled=True)


def layer(x, dy, wq, wk, wv, wo, w_gate, w_up, w_down):
    own, d = x.shape
    tp = lax.axis_size("tp")
    tokens, rows = own * tp, own // 2
    part = lambda t, j: t[j * rows : (j + 1) * rows]
    every = range(2)
    nq, nk = wq.shape[1], wk.shape[1]

    a_own = normed(x)
    a = [gather(part(a_own, j)) for j in every]
    w_qkv = jnp.concatenate([wq, wk, wv], 1)
    cos, sin = turn_by(tokens)
    qkv = [mm(t, w_qkv) for t in a]
    dy_all = [gather(after(part(dy, 0), qkv[0]))]
    heads, lse = attend(qkv, cos, sin, own)
    terms = [mm(t, wo) for t in heads]
    d_hidden = [mm(dy_all[0], w_down, 1, 1)]
    first = part(x, 0) + after(scatter(after(terms[0], dy_all[0])), d_hidden[0])
    b_first, back_first = jax.vjp(normed, first)
    second = part(x, 1) + after(scatter(terms[1]), b_first)
    b_second, back_second = jax.vjp(normed, second)
    b = [gather(b_first), gather(b_second)]
    dy_all.append(gather(after(part(dy, 1), b[0])))
    d_hidden.append(mm(dy_all[1], w_down, 1, 1))

    hidden, d_gate, d_up = (list(t) for t in zip(*(gated(b[j], w_gate, w_up, d_hidden[j], f"gated{j}") for j in every)))
    terms = [back_through([(d_gate[0], w_gate), (d_up[0], w_up)], "by_b0")]
    summed = scatter(after(terms[0], *b, *dy_all))
    dh = [part(dy, 0) + back_first(after(summed, d_gate[1]))[0]]
    dh_all = [gather(dh[0])]
    terms.append(back_through([(after(d_gate[1], dh[0]), w_gate), (d_up[1], w_up)], "by_b1"))
    summed = scatter(after(terms[1], dh_all[0]))
    (g_gate,) = weight_grads(b, [[d_gate[0], after(d_gate[1], terms[1])]], "g_gate", 512, 1280)
    dh.append(part(dy, 1) + back_second(after(summed, g_gate))[0])
    dh_all.append(gather(dh[1]))
    (g_up,) = weight_grads(b, [[d_up[0], after(d_up[1], dh[1])]], "g_up", 512, 1280)
    dh_all[1] = after(dh_all[1], g_up)

    d_heads = [mm(t, wo, 1, 1) for t in dh_all]
    d_qkv = attend_bwd(qkv, cos, sin, d_heads, heads, lse, own)
    terms = [back_through([(d_qkv[j], w_qkv)], f"by_a{j}") for j in every]
    by_a = [scatter(t) for t in terms]
    _, back_a = jax.vjp(normed, x)
    by_x = jnp.concatenate(dh, 0) + back_a(jnp.concatenate(by_a, 0))[0]
    columns = lambda at, n: [(t, at, n) for t in d_qkv]
    g_q, g_k, g_v = weight_grads(a, [columns(0, nq), columns(nq, nk), columns(nq + nk, nk)], "g_qkv", 512)
    (g_o,) = weight_grads(heads, [dh_all], "g_o", 896, 1024)
    (g_down,) = weight_grads([*hidden[:-1], after(hidden[-1], terms[-1])], [dy_all], "g_down", 512, 1792)
    return by_x, g_q, g_k, g_v, g_o, g_gate, g_up, g_down


def solution(mesh):
    def step(x, dy, *weights):
        by_x, *by_w = layer(x[0], dy[0], *weights)
        return (by_x[None], *by_w)

    states, by_columns, by_rows = P("dp", "tp", None), P(None, "tp"), P("tp", None)
    weights = (by_columns, by_columns, by_columns, by_rows, by_columns, by_columns, by_rows)
    own = tuple(P("dp", "tp") if spec == by_columns else P(("dp", "tp"), None) for spec in weights)
    return jax.shard_map(step, mesh=mesh, in_specs=(states, states, *weights), out_specs=(states, *own), check_vma=False)
```

```python
import functools

import jax
import jax.numpy as jnp
from jax import lax
from jax.experimental import pallas as pl
from jax.experimental.pallas import tpu as pltpu

NEG = -1e30
HIDDEN = 2 * NEG
LOG2E = 1.4426950408889634
VMEM = 56 * 2**20
STRIP = 512
HEAD = 128
BF = jnp.bfloat16
F32 = jnp.float32


def _fit(size, want, unit=128):
    return max(n for n in range(unit, max(min(want, size), unit) + 1, unit) if size % n == 0)


def _dot(a, b, ca, cb):
    return lax.dot_general(a, b, (((ca,), (cb,)), ((), ())), preferred_element_type=F32)


def _gap(bk, cols, bq):
    return lax.rem(lax.broadcasted_iota(jnp.int32, (bk, cols), 1), bq) - lax.broadcasted_iota(jnp.int32, (bk, cols), 0)


def _turn(t, cos, sin):
    wide = t.astype(F32)
    return (wide * cos + pltpu.roll(wide, HEAD // 2, 1) * sin).astype(BF)


def _runs(size, own, rows):
    return [(n * own + p * rows, p, n * rows) for n in range(size // own) for p in range(own // rows)]


def _load_keys(kv, cos_ref, sin_ref, k_s, v_s, own, rows):
    for at, p, there in _runs(k_s.shape[0], own, rows):
        here = slice(at, at + rows)
        k_s[here, :] = _turn(kv[2 * p][there : there + rows, :], cos_ref[here, :], sin_ref[here, :])
        v_s[here, :] = kv[2 * p + 1][there : there + rows, :]


def _load_queries(qs, cos_ref, sin_ref, q_s, bq, own, rows):
    first = pl.program_id(0) * bq
    for at, p, there in _runs(bq, own, rows):
        here = pl.ds(first + at, rows)
        cos, sin = cos_ref[here, :], sin_ref[here, :]
        for n in range(q_s.shape[0] // bq):
            q_s[n * bq + at : n * bq + at + rows, :] = _turn(qs[p][there : there + rows, n * HEAD : (n + 1) * HEAD], cos, sin)


def _row(ref):
    return jnp.concatenate([ref[n : n + 1, :] for n in range(ref.shape[0])], axis=1)


def _blocks(bq, bk, block):
    first = pl.program_id(0) * bq
    whole, last = lax.div(first + 1, bk), lax.div(first + bq - 1 + bk, bk)
    lax.fori_loop(0, whole, lambda j, _: block(j, False), None)
    lax.fori_loop(whole, last, lambda j, _: block(j, True), None)


def _forward(*refs, pieces, own, scale, bq, bk):
    qs, kv = refs[:pieces], refs[pieces : 3 * pieces]
    cos_ref, sin_ref = refs[3 * pieces : 3 * pieces + 2]
    outs, (lse_ref, q_s, k_s, v_s, top_s, mix_s, gap_s) = refs[3 * pieces + 2 : 4 * pieces + 2], refs[4 * pieces + 2 :]
    rows, g, cols = own // pieces, q_s.shape[0] // bq, q_s.shape[0]
    e = scale * LOG2E
    wide = _fit(cols, STRIP)
    strips = range(0, cols, wide)
    first_query = pl.program_id(0) * bq

    @pl.when(pl.program_id(0) == 0)
    def _():
        gap_s[...] = _gap(bk, cols, bq)
        _load_keys(kv, cos_ref, sin_ref, k_s, v_s, own, rows)

    _load_queries(qs, cos_ref, sin_ref, q_s, bq, own, rows)
    top_s[...] = jnp.full_like(top_s, NEG)
    mix_s[...] = jnp.zeros_like(mix_s)
    ones = jnp.ones((8, bk), BF)

    def block(j, masked):
        here = pl.ds(j * bk, bk)
        scores = [_dot(k_s[here, :], q_s[at : at + wide, :], 1, 1) for at in strips]
        ok = gap_s[...] >= j * bk - first_query if masked else None
        weights, keeps = [], []
        for at, s in zip(strips, scores):
            if masked:
                s = jnp.where(ok[:, at : at + wide], s, HIDDEN)
            old = top_s[:, at : at + wide]
            top = jnp.maximum(old, s.max(axis=0, keepdims=True))
            top_s[:, at : at + wide] = top
            weights.append(jnp.exp2((s - top) * e).astype(BF))
            keeps.append(jnp.exp2((old - top) * e))
        for at, p, keep in zip(strips, weights, keeps):
            values = jnp.concatenate([v_s[here, :].T, ones], axis=0)
            mix_s[:, at : at + wide] = mix_s[:, at : at + wide] * keep + _dot(values, p, 1, 0)

    _blocks(bq, bk, block)
    total = mix_s[HEAD : HEAD + 1, :]
    out = (mix_s[:HEAD, :] * (1 / total)).T.astype(BF)
    for at, p, there in _runs(bq, own, rows):
        for n in range(g):
            outs[p][there : there + rows, n * HEAD : (n + 1) * HEAD] = out[n * bq + at : n * bq + at + rows, :]
    lse = top_s[...] * scale + jnp.log(total)
    for n in range(g):
        lse_ref[n : n + 1, :] = lse[:, n * bq : (n + 1) * bq]


def _cost(g, tokens, dots):
    return pl.CostEstimate(flops=g * tokens * tokens * HEAD * dots, transcendentals=g * tokens * tokens // 2, bytes_accessed=8 * g * tokens * HEAD)


def _given(qkv, g, bq, tokens):
    share, size = bq // len(qkv), qkv[0].shape[0]
    specs = [pl.BlockSpec((share, g * HEAD), lambda i: (i, 0))] * len(qkv)
    specs += [pl.BlockSpec((size, HEAD), lambda i: (0, g)), pl.BlockSpec((size, HEAD), lambda i: (0, g + 1))] * len(qkv)
    return specs + [pl.BlockSpec((tokens, HEAD), lambda i: (0, 0))] * 2


def attend(qkv, cos, sin, own, bq=512, bk=512):
    pieces, tokens = len(qkv), cos.shape[0]
    g = qkv[0].shape[1] // HEAD - 2
    cols, share = g * bq, bq // pieces
    *heads, lse = pl.pallas_call(
        functools.partial(_forward, pieces=pieces, own=own, scale=HEAD**-0.5, bq=bq, bk=bk),
        grid=(tokens // bq,), in_specs=_given(qkv, g, bq, tokens),
        out_specs=[pl.BlockSpec((share, g * HEAD), lambda i: (i, 0))] * pieces + [pl.BlockSpec((g, bq), lambda i: (0, i))],
        out_shape=[jax.ShapeDtypeStruct((t.shape[0], g * HEAD), BF) for t in qkv] + [jax.ShapeDtypeStruct((g, tokens), F32)],
        scratch_shapes=[pltpu.VMEM((cols, HEAD), BF), pltpu.VMEM((tokens, HEAD), BF), pltpu.VMEM((tokens, HEAD), BF), pltpu.VMEM((1, cols), F32),
                        pltpu.VMEM((HEAD + 8, cols), F32), pltpu.VMEM((bk, cols), jnp.int32)],
        compiler_params=pltpu.CompilerParams(dimension_semantics=("arbitrary",), vmem_limit_bytes=VMEM),
        cost_estimate=_cost(g, tokens, 2), name="attend")(*qkv, *(t for t in qkv for _ in (0, 1)), cos, sin)
    return heads, lse


def _backward(*refs, pieces, own, scale, bq, bk):
    qs, kv = refs[:pieces], refs[pieces : 3 * pieces]
    cos_ref, sin_ref = refs[3 * pieces : 3 * pieces + 2]
    d_heads, heads = refs[3 * pieces + 2 : 4 * pieces + 2], refs[4 * pieces + 2 : 5 * pieces + 2]
    lse_ref, outs = refs[5 * pieces + 2], refs[5 * pieces + 3 : 6 * pieces + 3]
    q_s, k_s, v_s, do_s, delta_s, dq_s, dk_s, dv_s, gap_s = refs[6 * pieces + 3 :]
    rows, g, cols = own // pieces, q_s.shape[0] // bq, q_s.shape[0]
    e = scale * LOG2E
    wide = _fit(cols, STRIP)
    strips = range(0, cols, wide)
    step = pl.program_id(0)
    first_query = step * bq

    @pl.when(step == 0)
    def _():
        gap_s[...] = _gap(bk, cols, bq)
        _load_keys(kv, cos_ref, sin_ref, k_s, v_s, own, rows)
        dk_s[...] = jnp.zeros_like(dk_s)
        dv_s[...] = jnp.zeros_like(dv_s)

    _load_queries(qs, cos_ref, sin_ref, q_s, bq, own, rows)
    for n in range(g):
        for at, p, there in _runs(bq, own, rows):
            out, d_out = (t[p][there : there + rows, n * HEAD : (n + 1) * HEAD] for t in (heads, d_heads))
            here = slice(n * bq + at, n * bq + at + rows)
            do_s[here, :] = d_out
            delta_s[:, here] = (d_out.astype(F32) * out.astype(F32)).T.sum(axis=0, keepdims=True)
    dq_s[...] = jnp.zeros_like(dq_s)
    lses = _row(lse_ref) * LOG2E

    def block(j, masked):
        here = pl.ds(j * bk, bk)
        part_q = [q_s[at : at + wide, :] for at in strips]
        part_do = [do_s[at : at + wide, :] for at in strips]
        scores = [_dot(k_s[here, :], x, 1, 1) for x in part_q]
        dps = [_dot(v_s[here, :], x, 1, 1) for x in part_do]
        ok = gap_s[...] >= j * bk - first_query if masked else None
        for n, at in enumerate(strips):
            p = jnp.exp2(scores[n] * e - lses[:, at : at + wide])
            if masked:
                p = jnp.where(ok[:, at : at + wide], p, 0.0)
            ds = (p * (dps[n] - delta_s[:, at : at + wide])).astype(BF)
            dv_s[here, :] += _dot(p.astype(BF), part_do[n], 1, 0)
            dk_s[here, :] += _dot(ds, part_q[n], 1, 0)
            dq_s[:, at : at + wide] += _dot(k_s[here, :].T, ds, 1, 0)

    _blocks(bq, bk, block)
    dq = (dq_s[...] * scale).T.astype(BF)
    share = bq // pieces
    for at, p, there in _runs(bq, own, rows):
        here = pl.ds(first_query + at, rows)
        cos, sin = cos_ref[here, :], sin_ref[here, :]
        for n in range(g):
            outs[p][pl.ds(step * share + there, rows), n * HEAD : (n + 1) * HEAD] = _turn(dq[n * bq + at : n * bq + at + rows, :], cos, -sin)

    @pl.when(step == pl.num_programs(0) - 1)
    def _():
        for at, p, there in _runs(dk_s.shape[0], own, rows):
            here = slice(at, at + rows)
            dk = (dk_s[here, :] * scale).astype(BF)
            outs[p][there : there + rows, g * HEAD : (g + 1) * HEAD] = _turn(dk, cos_ref[here, :], -sin_ref[here, :])
            outs[p][there : there + rows, (g + 1) * HEAD :] = dv_s[here, :].astype(BF)


def attend_bwd(qkv, cos, sin, d_heads, heads, lse, own, bq=256, bk=512):
    pieces, tokens = len(qkv), cos.shape[0]
    g = qkv[0].shape[1] // HEAD - 2
    cols, share = g * bq, bq // pieces
    whole = pl.BlockSpec(qkv[0].shape, lambda i: (0, 0))
    return pl.pallas_call(
        functools.partial(_backward, pieces=pieces, own=own, scale=HEAD**-0.5, bq=bq, bk=bk),
        grid=(tokens // bq,),
        in_specs=_given(qkv, g, bq, tokens) + [pl.BlockSpec((share, g * HEAD), lambda i: (i, 0))] * (2 * pieces) + [pl.BlockSpec((g, bq), lambda i: (0, i))],
        out_specs=[whole] * pieces, out_shape=[jax.ShapeDtypeStruct(t.shape, BF) for t in qkv],
        scratch_shapes=[pltpu.VMEM((cols, HEAD), BF), pltpu.VMEM((tokens, HEAD), BF), pltpu.VMEM((tokens, HEAD), BF), pltpu.VMEM((cols, HEAD), BF),
                        pltpu.VMEM((1, cols), F32), pltpu.VMEM((HEAD, cols), F32), pltpu.VMEM((tokens, HEAD), F32), pltpu.VMEM((tokens, HEAD), F32),
                        pltpu.VMEM((bk, cols), jnp.int32)],
        compiler_params=pltpu.CompilerParams(dimension_semantics=("arbitrary",), vmem_limit_bytes=VMEM),
        cost_estimate=_cost(g, tokens, 5), name="attend_bwd")(*qkv, *(t for t in qkv for _ in (0, 1)), cos, sin, *d_heads, *heads, lse)


from jax.sharding import PartitionSpec as P

THETA = 10000
GRANT = 62 * 2**20


def normed(h):
    wide = h.astype(F32)
    scale = lax.rsqrt(jnp.mean(wide**2, -1, keepdims=True) + 1e-6)
    return (wide * scale).astype(BF)


def turn_by(tokens):
    half = HEAD // 2
    angle = jnp.arange(tokens, dtype=F32)[:, None] * THETA ** (-jnp.arange(half, dtype=F32) / half)
    cos, sin = jnp.cos(angle), jnp.sin(angle)
    return jnp.concatenate([cos, cos], 1), jnp.concatenate([-sin, sin], 1)


def mm(a, b, ca=1, cb=0):
    return _dot(a, b, ca, cb).astype(BF)


def _matmul_cost(m, n, k, times=1):
    return pl.CostEstimate(flops=2 * m * n * k * times, transcendentals=0, bytes_accessed=2 * times * (m * k + k * n + m * n))


def gated(b, w_gate, w_up, d_hidden, name, tm=512, tn=512):
    t, d = b.shape
    f = w_gate.shape[1]
    tm, tn = _fit(t, tm), _fit(f, tn)

    def kernel(b_ref, wg_ref, wu_ref, dh_ref, h_ref, dg_ref, du_ref):
        gate = jnp.dot(b_ref[...], wg_ref[...], preferred_element_type=F32)
        up = jnp.dot(b_ref[...], wu_ref[...], preferred_element_type=F32)
        dh = dh_ref[...].astype(F32)
        s = jax.nn.sigmoid(gate)
        act = gate * s
        h_ref[...] = (act * up).astype(BF)
        du_ref[...] = (dh * act).astype(BF)
        dg_ref[...] = (dh * up * (s + act * (1 - s))).astype(BF)

    out = pl.BlockSpec((tm, tn), lambda i, j: (i, j))
    w = pl.BlockSpec((d, tn), lambda i, j: (0, j))
    return pl.pallas_call(
        kernel, grid=(t // tm, f // tn), in_specs=[pl.BlockSpec((tm, d), lambda i, j: (i, 0)), w, w, out], out_specs=[out] * 3,
        out_shape=[jax.ShapeDtypeStruct((t, f), BF)] * 3, cost_estimate=_matmul_cost(t, f, d, 2), name=name,
        compiler_params=pltpu.CompilerParams(vmem_limit_bytes=GRANT, dimension_semantics=("parallel", "arbitrary")))(b, w_gate, w_up, d_hidden)


def back_through(pairs, name, tm=1024, tn=512):
    t, f = pairs[0][0].shape
    d = pairs[0][1].shape[0]
    n = len(pairs)
    tm, tn = _fit(t, tm), _fit(d, tn)

    def kernel(*refs):
        total = None
        for g, w in zip(refs[:n], refs[n : 2 * n]):
            term = _dot(g[...], w[...], 1, 1)
            total = term if total is None else total + term
        refs[2 * n][...] = total.astype(BF)

    return pl.pallas_call(
        kernel, grid=(t // tm, d // tn),
        in_specs=[pl.BlockSpec((tm, f), lambda i, j: (i, 0))] * n + [pl.BlockSpec((tn, f), lambda i, j: (j, 0))] * n,
        out_specs=pl.BlockSpec((tm, tn), lambda i, j: (i, j)), out_shape=jax.ShapeDtypeStruct((t, d), BF),
        cost_estimate=_matmul_cost(t, d, f, n), name=name,
        compiler_params=pltpu.CompilerParams(vmem_limit_bytes=GRANT, dimension_semantics=("parallel", "arbitrary")))(
            *(g for g, _ in pairs), *(w for _, w in pairs))


def weight_grads(pieces, lists, name, tm, tn=None):
    c, (t, m) = len(pieces), pieces[0].shape
    k = len(lists)
    widths = [bs[0][2] if isinstance(bs[0], tuple) else bs[0].shape[1] for bs in lists]
    tm = _fit(m, tm)
    tns = widths if tn is None else [_fit(n, tn) for n in widths]

    def kernel(*refs):
        ours, theirs, outs = refs[:c], refs[c : c + c * k], refs[c + c * k :]
        for l, out in enumerate(outs):
            total = None
            for i in range(c):
                term = _dot(ours[i][...], theirs[l * c + i][...], 0, 0)
                total = term if total is None else total + term
            out[...] = total.astype(BF)

    specs, given = [pl.BlockSpec((t, tm), lambda j, i: (0, i))] * c, list(pieces)
    for b, tn in ((b, tn) for bs, tn in zip(lists, tns) for b in bs):
        if not isinstance(b, tuple):
            specs.append(pl.BlockSpec((t, tn), lambda j, i: (0, j)))
            given.append(b)
        else:
            specs.append(pl.BlockSpec((t, tn), lambda j, i, at=b[1] // tn: (0, at)))
            given.append(b[0])
    return pl.pallas_call(
        kernel, grid=(widths[0] // tns[0], m // tm), in_specs=specs, out_specs=[pl.BlockSpec((tm, tn), lambda j, i: (i, j)) for tn in tns],
        out_shape=[jax.ShapeDtypeStruct((m, n), BF) for n in widths], cost_estimate=_matmul_cost(m, sum(widths), c * t), name=name,
        compiler_params=pltpu.CompilerParams(vmem_limit_bytes=GRANT, dimension_semantics=("parallel", "arbitrary")))(*given)


def after(value, *others):
    return lax.optimization_barrier((value, *others))[0]


def gather(rows):
    return lax.all_gather(rows, "tp", axis=0, tiled=True)


def scatter(terms):
    return lax.psum_scatter(terms, "tp", scatter_dimension=0, tiled=True)


def layer(x, dy, wq, wk, wv, wo, w_gate, w_up, w_down):
    own, d = x.shape
    tp = lax.axis_size("tp")
    tokens, rows = own * tp, own // 2
    part = lambda t, j: t[j * rows : (j + 1) * rows]
    every = range(2)
    nq, nk = wq.shape[1], wk.shape[1]

    a_own = normed(x)
    a = [gather(part(a_own, j)) for j in every]
    w_qkv = jnp.concatenate([wq, wk, wv], 1)
    cos, sin = turn_by(tokens)
    qkv = [mm(t, w_qkv) for t in a]
    dy_all = [gather(after(part(dy, 0), qkv[0]))]
    heads, lse = attend(qkv, cos, sin, own)
    terms = [mm(t, wo) for t in heads]
    d_hidden = [mm(dy_all[0], w_down, 1, 1)]
    first = part(x, 0) + after(scatter(after(terms[0], dy_all[0])), d_hidden[0])
    b_first, back_first = jax.vjp(normed, first)
    b = [gather(b_first)]
    summed = scatter(after(terms[1], b_first))
    dy_all.append(gather(after(part(dy, 1), b[0])))
    gate_unit = lambda j: gated(b[j], w_gate, w_up, d_hidden[j], f"gated{j}")
    units = [gate_unit(0)]
    second = part(x, 1) + after(summed, units[0][1])
    b_second, back_second = jax.vjp(normed, second)
    b.append(gather(b_second))

    d_hidden.append(mm(dy_all[1], w_down, 1, 1))
    b[1] = after(b[1], d_hidden[1])
    units.append(gate_unit(1))
    hidden, d_gate, d_up = (list(t) for t in zip(*units))
    terms = [back_through([(after(d_gate[0], b_second), w_gate), (d_up[0], w_up)], "by_b0")]
    summed = scatter(after(terms[0], *b, d_hidden[1]))
    dh = [part(dy, 0) + back_first(after(summed, d_gate[1]))[0]]
    dh_all = [gather(dh[0])]
    terms.append(back_through([(after(d_gate[1], dh[0]), w_gate), (d_up[1], w_up)], "by_b1"))
    summed = scatter(after(terms[1], dh_all[0]))
    (g_gate,) = weight_grads(b, [[d_gate[0], after(d_gate[1], terms[1])]], "g_gate", 1024, 1280)
    d_heads = [mm(dh_all[0], wo, 1, 1)]
    dh.append(part(dy, 1) + back_second(after(summed, g_gate, d_heads[0]))[0])
    dh_all.append(gather(dh[1]))
    (g_up,) = weight_grads(b, [[d_up[0], after(d_up[1], dh[1])]], "g_up", 1024, 1280)
    dh_all[1] = after(dh_all[1], g_up)

    d_heads.append(mm(dh_all[1], wo, 1, 1))
    d_qkv = attend_bwd(qkv, cos, sin, d_heads, heads, lse, own)
    terms = [back_through([(d_qkv[j], w_qkv)], f"by_a{j}", tn=1024) for j in every]
    by_a = [scatter(t) for t in terms]
    _, back_a = jax.vjp(normed, x)
    by_x = jnp.concatenate(dh, 0) + back_a(jnp.concatenate(by_a, 0))[0]
    columns = lambda at, n: [(t, at, n) for t in d_qkv]
    g_q, g_k, g_v = weight_grads(a, [columns(0, nq), columns(nq, nk), columns(nq + nk, nk)], "g_qkv", 1024)
    (g_o,) = weight_grads(heads, [dh_all], "g_o", 896, 1024)
    (g_down,) = weight_grads([*hidden[:-1], after(hidden[-1], terms[-1])], [dy_all], "g_down", 640, 1792)
    return by_x, g_q, g_k, g_v, g_o, g_gate, g_up, g_down


def solution(mesh):
    def step(x, dy, *weights):
        by_x, *by_w = layer(x[0], dy[0], *weights)
        return (by_x[None], *by_w)

    states, by_columns, by_rows = P("dp", "tp", None), P(None, "tp"), P("tp", None)
    weights = (by_columns, by_columns, by_columns, by_rows, by_columns, by_columns, by_rows)
    own = tuple(P("dp", "tp") if spec == by_columns else P(("dp", "tp"), None) for spec in weights)
    return jax.shard_map(step, mesh=mesh, in_specs=(states, states, *weights), out_specs=(states, *own), check_vma=False)
```
